32 devices in a mesh: tp: 32 (over z, y, x, core).
Axes of the slice: x: 2, y: 2, z: 4, core: 2. Of those that a mesh axis runs over, the one named last changes fastest.
Arguments:
- hidden: bfloat16 [3, 2048, 4096], P(None, 'tp')
- labels: int32 [3, 2048], P(None, 'tp')
- loss_mask: int32 [3, 2048], P(None, 'tp')
- norm_gain: float32 [4096], replicated
- w_head: bfloat16 [4096, 65536], P(None, 'tp')
Outputs:
- output 1: float32 [], replicated
- output 2: bfloat16 [3, 2048, 4096], P(None, 'tp')
- output 3: bfloat16 [4096, 65536], P(None, 'tp')
- output 4: float32 [4096], replicated
All inputs are finite; a program needn't handle non-finite values.
Results may differ from the reference program's by a relative error of at most 0.00839355.
Values are sent between devices in bfloat16 or wider.
A program may use at most 1 GiB of HBM per device.

```python
import jax
import jax.numpy as jnp
from jax import lax

BATCH_SIZE = 3
SEQ_DEV = 64
D_MODEL = 4096
VOCAB_SIZE = 65536
SHARDS = 32
SEQ_LEN = SEQ_DEV * SHARDS
VSHARD = VOCAB_SIZE // SHARDS
NORM_EPS = 1e-6
LOGIT_STD = 3.0
LABEL_PULL = 2.0


def draw_targets(route_key):
    key_hot, key_pick, key_uni, key_loc, key_rate, key_keep = jax.random.split(route_key, 6)
    hot_block = jax.random.randint(key_hot, (), 0, SHARDS)
    use_hot = jax.random.randint(key_pick, (BATCH_SIZE, SEQ_LEN), 0, 2)
    spread_ids = jax.random.randint(key_uni, (BATCH_SIZE, SEQ_LEN), 0, VOCAB_SIZE)
    hot_ids = hot_block * VSHARD + jax.random.randint(key_loc, (BATCH_SIZE, SEQ_LEN), 0, VSHARD)
    labels = jnp.where(use_hot == 1, hot_ids, spread_ids).astype(jnp.int32)
    keep_rate = jax.random.randint(key_rate, (BATCH_SIZE, SHARDS, 1), 1, 9)
    keep_draw = jax.random.randint(key_keep, (BATCH_SIZE, SHARDS, SEQ_DEV), 0, 8)
    loss_mask = (keep_draw < keep_rate).astype(jnp.int32).reshape(BATCH_SIZE, SEQ_LEN)
    first_pos = (jnp.arange(SEQ_LEN) == 0).astype(jnp.int32)
    loss_mask = jnp.maximum(loss_mask, first_pos[None, :])
    return labels, loss_mask


def setup_inputs(seed: int = 0) -> dict:
    root_key = jax.random.key(seed)
    key_route, key_head, key_noise, key_row, key_gain = jax.random.split(root_key, 5)
    labels, loss_mask = draw_targets(key_route)
    w_f32 = jax.random.normal(key_head, (D_MODEL, VOCAB_SIZE), jnp.float32) * (LOGIT_STD * D_MODEL ** -0.5)
    label_dirs = jnp.moveaxis(jnp.take(w_f32, labels, axis=1), 0, -1) * (D_MODEL ** 0.5 / LOGIT_STD)
    noise = jax.random.normal(key_noise, (BATCH_SIZE, SEQ_LEN, D_MODEL), jnp.float32)
    row_scale = jax.random.uniform(key_row, (BATCH_SIZE, SEQ_LEN, 1), jnp.float32, 0.5, 2.0)
    hidden = (row_scale * (noise + LABEL_PULL * D_MODEL ** -0.5 * label_dirs)).astype(jnp.bfloat16)
    norm_gain = 1.0 + 0.4 * jax.random.normal(key_gain, (D_MODEL,), jnp.float32)
    return {'hidden': hidden, 'labels': labels, 'loss_mask': loss_mask, 'norm_gain': norm_gain, 'w_head': w_f32.astype(jnp.bfloat16)}


def rms_norm(x_rows, norm_gain):
    inv_rms = lax.rsqrt(jnp.mean(x_rows * x_rows, axis=-1, keepdims=True) + NORM_EPS)
    return x_rows * inv_rms * norm_gain


def reference(hidden, labels, loss_mask, norm_gain, w_head):
    tokens = BATCH_SIZE * SEQ_LEN
    n_blocks = tokens // SEQ_DEV
    x_rows = hidden.reshape(tokens, D_MODEL).astype(jnp.float32)
    norm_out, norm_vjp = jax.vjp(rms_norm, x_rows, norm_gain)
    hn_rows = norm_out.astype(jnp.bfloat16)
    hn_cols = hn_rows.T
    label_ids = labels.reshape(tokens)
    tok_weight = loss_mask.reshape(tokens).astype(jnp.float32)
    kept_count = jnp.sum(tok_weight)

    def token_stats(blk_pair):
        hn_blk, lab_blk = blk_pair
        logits = jnp.dot(hn_blk, w_head, preferred_element_type=jnp.float32)
        row_max = jnp.max(logits, axis=-1)
        blk_norm = row_max + jnp.log(jnp.sum(jnp.exp(logits - row_max[:, None]), axis=-1))
        blk_label = jnp.take_along_axis(logits, lab_blk[:, None], axis=-1)[:, 0]
        return blk_norm, blk_label

    log_norm, label_logit = lax.map(token_stats, (hn_rows.reshape(n_blocks, SEQ_DEV, D_MODEL), label_ids.reshape(n_blocks, SEQ_DEV)))
    log_norm = log_norm.reshape(tokens)
    label_logit = label_logit.reshape(tokens)
    mean_loss = jnp.sum(tok_weight * (log_norm - label_logit)) / kept_count
    tok_scale = tok_weight / kept_count
    w_blocks = jnp.transpose(w_head.reshape(D_MODEL, SHARDS, VSHARD), (1, 0, 2))

    def shard_step(d_norm, shard_in):
        w_blk, shard_idx = shard_in
        logits = jnp.dot(hn_rows, w_blk, preferred_element_type=jnp.float32)
        col_ids = shard_idx * VSHARD + jnp.arange(VSHARD)
        is_label = (label_ids[:, None] == col_ids[None, :]).astype(jnp.float32)
        d_logits = ((jnp.exp(logits - log_norm[:, None]) - is_label) * tok_scale[:, None]).astype(jnp.bfloat16)
        d_blk = jnp.dot(hn_cols, d_logits, preferred_element_type=jnp.float32).astype(jnp.bfloat16)
        dhn_part = jnp.dot(d_logits, w_blk.T, preferred_element_type=jnp.float32).astype(jnp.bfloat16)
        return d_norm + dhn_part.astype(jnp.float32), d_blk

    d_norm, d_blocks = lax.scan(shard_step, jnp.zeros((tokens, D_MODEL), jnp.float32), (w_blocks, jnp.arange(SHARDS)))
    d_head = jnp.transpose(d_blocks, (1, 0, 2)).reshape(D_MODEL, VOCAB_SIZE)
    d_x, d_gain = norm_vjp(d_norm)
    d_hidden = d_x.astype(jnp.bfloat16).reshape(BATCH_SIZE, SEQ_LEN, D_MODEL)
    return mean_loss, d_hidden, d_head, d_gain
```

```python
import jax
import jax.numpy as jnp
from jax import lax
from jax.sharding import PartitionSpec as P

NORM_EPS = 1e-6


def rms_norm(x_rows, norm_gain):
    inv_rms = lax.rsqrt(jnp.mean(x_rows * x_rows, axis=-1, keepdims=True) + NORM_EPS)
    return x_rows * inv_rms * norm_gain


def solution(mesh):
    n = mesh.shape['tp']
    dims = (n // 8, 2, 2, 2)

    def swap(a, bits):
        return lax.ppermute(a, 'tp', [(i, i ^ bits) for i in range(n)])

    def device_step(hidden, labels, loss_mask, norm_gain, w_head):
        f32 = jnp.float32
        batch_size, seq_loc, model_width = hidden.shape
        v_loc = w_head.shape[1]
        me = lax.axis_index('tp')
        core, x, y, z = me & 1, (me >> 1) & 1, (me >> 2) & 1, me >> 3
        norm_loc, norm_vjp = jax.vjp(rms_norm, hidden.astype(f32), norm_gain)
        hn_loc = norm_loc.astype(jnp.bfloat16)
        hn = [lax.all_gather(hn_loc[b], 'tp', axis=0, tiled=True) for b in range(2)]
        packed = lax.all_gather(labels * 2 + loss_mask, 'tp', axis=1, tiled=True)
        label_all, mask_all = packed >> 1, packed & 1
        tok_weight = mask_all.astype(f32)
        kept_count = jnp.sum(tok_weight)
        tok_scale = tok_weight / kept_count
        cols = lax.broadcasted_iota(jnp.int32, (1, v_loc), 1) + me * v_loc

        logits, is_label, stats = [], [], []

        def forward(b):
            lg = jnp.einsum('td,dv->tv', hn[b], w_head, preferred_element_type=f32)
            hit = cols == label_all[b][:, None]
            row_max = jnp.max(lg, axis=-1)
            row_sum = jnp.sum(jnp.exp(lg - row_max[:, None]), axis=-1)
            row_lab = jnp.sum(jnp.where(hit, lg, 0.0), axis=-1)
            logits.append(lg)
            is_label.append(hit)
            mine = jnp.stack([row_max, row_sum, row_lab, tok_weight[b]])
            if b == 0:
                mine, last = lax.optimization_barrier((mine, hn_loc[2]))
                stats.append(lax.all_gather(mine, 'tp', axis=0, tiled=False))
                hn.append(lax.all_gather(last, 'tp', axis=0, tiled=True))
            else:
                stats.append(lax.all_gather(mine, 'tp', axis=0, tiled=False))

        log_norm, label_logit, d_logits = [], [], []

        def softmax_grad(b):
            mx, sm, lb = stats[b][:, 0], stats[b][:, 1], stats[b][:, 2]
            top = jnp.max(mx, axis=0)
            log_norm.append(top + jnp.log(jnp.sum(sm * jnp.exp(mx - top), axis=0)))
            label_logit.append(jnp.sum(lb, axis=0))
            d_logits.append(((jnp.exp(logits[b] - log_norm[b][:, None]) - is_label[b].astype(f32)) * tok_scale[b][:, None]).astype(jnp.bfloat16))

        def at(a, axis, i):
            return lax.dynamic_index_in_dim(a, i, axis, keepdims=False)

        def after(values, dep):
            return lax.optimization_barrier((values, dep))[0]

        class Reduce:
            def __init__(self, part, first):
                part = part.reshape(*dims, seq_loc, -1)
                if first == 'x':
                    a_bit, a_axis, a_i, self.bit, self.i = 2, 2, x, 4, y
                else:
                    a_bit, a_axis, a_i, self.bit, self.i = 4, 1, y, 2, x

                def group(da, dc):
                    return at(at(part, 3, core ^ dc), a_axis, a_i ^ da)

                got = [swap(group(1, 0), a_bit), swap(group(1, 1), a_bit | 1), swap(group(0, 1), 1)]
                self.terms = [group(0, 0)] + got

            def second(self, dep):
                terms = after(self.terms, dep)

                def total(db):
                    return sum(at(t, 1, self.i ^ db).astype(f32) for t in terms)

                self.terms = [total(0), swap(total(1), self.bit)]

            def third(self, dep):
                half = sum(after(self.terms, dep))
                self.terms = [at(half, 0, z)] + [swap(at(half, 0, z ^ dz), dz * 8) for dz in range(1, dims[0])]

            def last(self, dep):
                return sum(after(self.terms, dep))

        h = model_width // 2
        units = {}

        def hidden_grad(b):
            for k, first in enumerate(('x', 'y')):
                part = jnp.einsum('tv,dv->td', d_logits[b], w_head[k * h:(k + 1) * h], preferred_element_type=f32).astype(jnp.bfloat16)
                units[b, k] = Reduce(part, first)
            return part

        def head_grad(b, acc):
            term = jnp.einsum('td,tv->dv', hn[b], d_logits[b], preferred_element_type=f32)
            return term if acc is None else acc + term

        forward(0)
        forward(1)
        softmax_grad(0)
        done = hidden_grad(0)
        logits[1], hn[2] = after((logits[1], hn[2]), done)
        forward(2)
        logits[1] = after(logits[1], logits[2])
        softmax_grad(1)
        done = hidden_grad(1)
        for k in range(2):
            units[0, k].second(done)
        d_logits[0] = after(d_logits[0], done)
        head = head_grad(0, None)
        logits[2] = after(logits[2], head)
        softmax_grad(2)
        for k in range(2):
            units[1, k].second(d_logits[2])
        done = hidden_grad(2)
        for k in range(2):
            units[0, k].third(done)
        d_logits[1] = after(d_logits[1], done)
        head = head_grad(1, head)
        for k in range(2):
            units[1, k].third(head)
            units[2, k].second(head)
        d_logits[2] = after(d_logits[2], head)
        head = head_grad(2, head)
        d_head = head.astype(jnp.bfloat16)
        for k in range(2):
            units[2, k].third(d_head)
        d_norm = [jnp.concatenate([units[b, k].last(d_head) for k in range(2)], axis=-1) for b in range(batch_size)]
        loss = sum(jnp.sum(tok_weight[b] * (log_norm[b] - label_logit[b])) for b in range(batch_size))
        mean_loss = loss / kept_count
        d_x, d_gain = norm_vjp(jnp.stack(d_norm))
        d_gain = lax.psum(d_gain, 'tp')
        return mean_loss, d_x.astype(jnp.bfloat16), d_head, d_gain

    return jax.shard_map(device_step, mesh=mesh, in_specs=(P(None, 'tp', None), P(None, 'tp'), P(None, 'tp'), P(), P(None, 'tp')), out_specs=(P(), P(None, 'tp', None), P(None, 'tp'), P()), check_vma=False)
```

```python
import jax
import jax.numpy as jnp
from jax import lax
from jax.sharding import PartitionSpec as P

NORM_EPS = 1e-6
STAGES = ((1, 96), (2, 64), (4, 48), (8, 32))
ROWS = 128
CHUNKS = 2
UNITS = ((('y', 'z', 'x'), 6), (('x', 'z', 'y'), 6), (('x', 'y', 'z'), 10), (('y', 'x', 'z'), 10))


def rms_norm(x_rows, norm_gain):
    inv_rms = lax.rsqrt(jnp.mean(x_rows * x_rows, axis=-1, keepdims=True) + NORM_EPS)
    return x_rows * inv_rms * norm_gain


def full_step(n_shards, hidden, labels, loss_mask, norm_gain, w_head):
    batch_size, seq_loc, model_width = hidden.shape
    v_loc = w_head.shape[1]
    norm_loc, norm_vjp = jax.vjp(rms_norm, hidden.astype(jnp.float32), norm_gain)
    hn_all = lax.all_gather(norm_loc.astype(jnp.bfloat16), 'tp', axis=1, tiled=True)
    label_all = lax.all_gather(labels, 'tp', axis=1, tiled=True)
    mask_all = lax.all_gather(loss_mask, 'tp', axis=1, tiled=True)
    logits = jnp.einsum('btd,dv->btv', hn_all, w_head, preferred_element_type=jnp.float32)
    row_max = lax.pmax(jnp.max(logits, axis=-1), 'tp')
    sum_exp = lax.psum(jnp.sum(jnp.exp(logits - row_max[..., None]), axis=-1), 'tp')
    col_start = lax.axis_index('tp') * v_loc
    is_label = (lax.broadcasted_iota(jnp.int32, (1, 1, v_loc), 2) + col_start) == label_all[..., None]
    label_logit = lax.psum(jnp.sum(jnp.where(is_label, logits, 0.0), axis=-1), 'tp')
    log_norm = row_max + jnp.log(sum_exp)
    tok_weight = mask_all.astype(jnp.float32)
    kept_count = jnp.sum(tok_weight)
    mean_loss = jnp.sum(tok_weight * (log_norm - label_logit)) / kept_count
    tok_scale = tok_weight / kept_count
    d_logits = ((jnp.exp(logits - log_norm[..., None]) - is_label.astype(jnp.float32)) * tok_scale[..., None]).astype(jnp.bfloat16)
    d_head = jnp.einsum('btd,btv->dv', hn_all, d_logits, preferred_element_type=jnp.float32).astype(jnp.bfloat16)
    dhn_part = jnp.einsum('btv,dv->btd', d_logits, w_head, preferred_element_type=jnp.float32).astype(jnp.bfloat16)
    received = lax.all_to_all(dhn_part.reshape(batch_size, n_shards, seq_loc, model_width), 'tp', 1, 1, tiled=True)
    d_norm = jnp.sum(received, axis=1, dtype=jnp.float32)
    d_x, d_gain = norm_vjp(d_norm)
    d_gain = lax.psum(d_gain, 'tp')
    return mean_loss, d_x.astype(jnp.bfloat16), d_head, d_gain


def solution(mesh):
    n = mesh.shape['tp']
    dims = (n // 8, 2, 2, 2)
    bits = [1 << i for i in range(n.bit_length() - 1)]

    def swap(a, flip):
        return lax.ppermute(a, 'tp', [(i, i ^ flip) for i in range(n)])

    def at(a, axis, i):
        return lax.dynamic_index_in_dim(a, i, axis, keepdims=False)

    def after(values, dep):
        return lax.optimization_barrier((values, dep))[0]

    def device_step(hidden, labels, loss_mask, norm_gain, w_head):
        f32, i32 = jnp.float32, jnp.int32
        batch_size, seq_loc, model_width = hidden.shape
        n_rows = batch_size * seq_loc
        v_loc = w_head.shape[1]
        me = lax.axis_index('tp')
        place = {'core': me & 1, 'x': (me >> 1) & 1, 'y': (me >> 2) & 1, 'z': me >> 3}
        slot = jnp.arange(n_rows, dtype=i32)

        mask = loss_mask.reshape(n_rows)
        pos = jnp.cumsum(mask) - 1
        count = jnp.sum(mask)
        chosen = (pos[None, :] == slot[:, None]) & (mask[None, :] == 1)
        order = jnp.sum(jnp.where(chosen, slot[None, :], 0), axis=1)
        lab = jnp.sum(jnp.where(chosen, labels.reshape(n_rows)[None, :], 0), axis=1)
        rows = jnp.take(hidden.reshape(n_rows, model_width), order, axis=0, mode='clip')
        fits = jnp.bool_(True)
        moves = []
        for bit, cap in STAGES:
            start = jnp.maximum(count - cap, 0)
            ints = jnp.concatenate([lax.dynamic_slice_in_dim(lab, start, cap), jnp.full((128,), count, i32)])
            got_rows = swap(lax.dynamic_slice_in_dim(rows, start, cap), bit)
            got_ints = swap(ints, bit)
            other = got_ints[cap]
            upper = (me & bit) // bit
            target = (count + other + 1 - upper) >> 1
            fits = fits & (jnp.abs(target - count) <= cap)
            first = count + other - target - jnp.maximum(other - cap, 0)
            src = jnp.where(slot < count, slot, n_rows + jnp.clip(first + slot - count, 0, cap - 1))
            rows = jnp.take(jnp.concatenate([rows, got_rows]), src, axis=0, mode='clip')
            lab = jnp.take(jnp.concatenate([lab, got_ints[:cap]]), src, axis=0, mode='clip')
            moves.append((bit, cap, count, other, target))
            count = target
        fits = fits & (count <= ROWS)
        x_rows, lab = rows[:ROWS], jnp.where(slot < count, lab, -1)[:ROWS]

        norm_loc, norm_vjp = jax.vjp(rms_norm, x_rows.astype(f32), norm_gain)
        hn_loc = norm_loc.astype(jnp.bfloat16)
        per = ROWS // CHUNKS
        hn = [lax.all_gather(hn_loc[c * per:(c + 1) * per], 'tp', axis=0, tiled=True) for c in range(CHUNKS)]
        known = lax.all_gather(jnp.concatenate([lab, jnp.full((128,), fits.astype(i32))]), 'tp', axis=0, tiled=False)
        all_fit = jnp.min(known[:, ROWS]) == 1
        label_all = [known[:, c * per:(c + 1) * per].reshape(n * per) for c in range(CHUNKS)]
        weight = [(lb >= 0).astype(f32) for lb in label_all]
        kept_count = sum(jnp.sum(w) for w in weight)
        cols = lax.broadcasted_iota(i32, (1, v_loc), 1) + me * v_loc

        def forward(c):
            lg = jnp.einsum('td,dv->tv', hn[c], w_head, preferred_element_type=f32)
            lg = lax.optimization_barrier(lg)
            row_max = jnp.max(lg, axis=-1)
            row_sum = jnp.sum(jnp.exp(lg - row_max[:, None]), axis=-1)
            row_lab = jnp.sum(jnp.where(cols == label_all[c][:, None], lg, 0.0), axis=-1)
            return lg, jnp.stack([row_max, row_sum, row_lab])

        def combine(mine):
            for bit in bits:
                theirs = swap(mine, bit)
                upper = (me & bit) != 0
                lo, hi = jnp.where(upper, theirs, mine), jnp.where(upper, mine, theirs)
                top = jnp.maximum(lo[0], hi[0])
                mine = jnp.stack([top, lo[1] * jnp.exp(lo[0] - top) + hi[1] * jnp.exp(hi[0] - top), lo[2] + hi[2]])
            return mine[0] + jnp.log(mine[1]), mine[2]

        def softmax_grad(c, lg, log_norm):
            is_label = (cols == label_all[c][:, None]).astype(f32)
            scale = weight[c] / kept_count
            return ((jnp.exp(lg - log_norm[:, None]) - is_label) * scale[:, None]).astype(jnp.bfloat16)

        class Reduce:
            def __init__(self, part, path):
                part = part.reshape(*dims, per, -1)
                step = {'x': 2, 'y': 4}
                a, self.second_axis, self.third_axis = path
                a_axis = {'y': 1, 'x': 2}[a]
                self.bit = {**step, 'z': 8}

                def group(da, dc):
                    return at(at(part, 3, place['core'] ^ dc), a_axis, place[a] ^ da)

                self.sent = [group(1, 0), group(1, 1), group(0, 1)]
                self.terms = [group(0, 0)]
                self.terms += [swap(g, f) for g, f in zip(self.sent, (step[a], step[a] | 1, 1))]

            def _exchange(self, pick, name):
                size = dims[0] if name == 'z' else 2
                self.sent = [pick(place[name] ^ d) for d in range(1, size)]
                self.terms = [pick(place[name])]
                self.terms += [swap(g, self.bit[name] * d) for d, g in enumerate(self.sent, 1)]
                return self.sent

            def second(self, dep):
                terms, name = after(self.terms, dep), self.second_axis
                axis = 0 if name == 'z' else 1
                return self._exchange(lambda i: sum(at(t, axis, i).astype(f32) for t in terms), name)

            def third(self, dep):
                terms = after(self.terms, dep)
                return self._exchange(lambda i: sum(at(t, 0, i) for t in terms), self.third_axis)

            def last(self, dep):
                return sum(after(self.terms, dep))

        d_logits, log_norm, label_logit, units = {}, {}, {}, {}

        def hidden_grad(c, u, dep):
            low = sum(w for _, w in UNITS[:u]) * model_width // 32
            path, w = UNITS[u]
            dl, w_part = after(d_logits[c], dep), w_head[low:low + w * model_width // 32]
            part = jnp.einsum('tv,dv->td', dl, w_part, preferred_element_type=f32).astype(jnp.bfloat16)
            units[c, u] = Reduce(part, path)
            return units[c, u].sent

        def head_grad(c, acc, dep):
            dl = after(d_logits[c], dep)
            term = jnp.einsum('td,tv->dv', hn[c], dl, preferred_element_type=f32)
            return term if acc is None else acc + term

        nu = len(UNITS)
        lg0, st0 = forward(0)
        log_norm[0], label_logit[0] = combine(st0)
        d_logits[0] = softmax_grad(0, lg0, log_norm[0])
        dep = d_logits[0]
        for u in range(nu):
            dep = hidden_grad(0, u, dep)
        hn[1] = after(hn[1], dep)
        lg1, st1 = forward(1)
        for u in range(2):
            dep = units[0, u].second(st1)
        log_norm[1], label_logit[1] = combine(after(st1, dep))
        lg1 = after(lg1, log_norm[1])
        d_logits[1] = dep = softmax_grad(1, lg1, log_norm[1])
        for u in range(2, nu):
            dep = units[0, u].second(dep)
        for u in range(nu):
            dep = hidden_grad(1, u, dep)
        for u in range(2):
            dep = units[0, u].third(dep)
        head = dep = head_grad(0, None, dep)
        for u in range(2):
            dep = units[1, u].second(dep)
        for u in range(2, nu):
            dep = units[0, u].third(dep)
        for u in range(2, nu):
            dep = units[1, u].second(dep)
        d_head = dep = head_grad(1, head, dep).astype(jnp.bfloat16)
        for u in range(nu):
            dep = units[1, u].third(dep)
        d_norm = jnp.concatenate([jnp.concatenate([units[c, u].last(dep) for u in range(nu)], axis=-1) for c in range(CHUNKS)])
        loss = sum(jnp.sum(weight[c] * (log_norm[c] - label_logit[c])) for c in range(CHUNKS))
        mean_loss = loss / kept_count
        d_x, d_gain = norm_vjp(d_norm)
        for bit in bits:
            d_gain = d_gain + swap(d_gain, bit)

        back = jnp.concatenate([d_x.astype(jnp.bfloat16), jnp.zeros((n_rows - ROWS, model_width), jnp.bfloat16)])
        for bit, cap, count, other, target in reversed(moves):
            got = swap(lax.dynamic_slice_in_dim(back, jnp.minimum(count, n_rows - cap), cap), bit)
            first = jnp.maximum(other - (n_rows - cap), 0)
            src = jnp.where(slot < target, slot, n_rows + jnp.clip(first + slot - target, 0, cap - 1))
            back = jnp.take(jnp.concatenate([back, got]), src, axis=0, mode='clip')
        back = jnp.where(mask[:, None] == 1, jnp.take(back, pos, axis=0, mode='clip'), jnp.zeros((), jnp.bfloat16))
        d_hidden = back.reshape(hidden.shape)
        return lax.cond(
            all_fit,
            lambda: (mean_loss, d_hidden, d_head, d_gain),
            lambda: full_step(n, hidden, labels, loss_mask, norm_gain, w_head),
        )

    return jax.shard_map(device_step, mesh=mesh, in_specs=(P(None, 'tp', None), P(None, 'tp'), P(None, 'tp'), P(), P(None, 'tp')), out_specs=(P(), P(None, 'tp', None), P(None, 'tp'), P()), check_vma=False)
```

```python
import jax
import jax.numpy as jnp
from jax import lax
from jax.sharding import PartitionSpec as P

NORM_EPS = 1e-6
STAGES = ((1, 64), (2, 56), (4, 40), (8, 32), (16, 24))
ROWS = (64, 56)
UNITS = ((('y', 'z', 'x'), 6), (('x', 'z', 'y'), 6), (('x', 'y', 'z'), 10), (('y', 'x', 'z'), 10))


def rms_norm(x_rows, norm_gain):
    inv_rms = lax.rsqrt(jnp.mean(x_rows * x_rows, axis=-1, keepdims=True) + NORM_EPS)
    return x_rows * inv_rms * norm_gain


def full_step(n_shards, hidden, labels, loss_mask, norm_gain, w_head):
    batch_size, seq_loc, model_width = hidden.shape
    v_loc = w_head.shape[1]
    norm_loc, norm_vjp = jax.vjp(rms_norm, hidden.astype(jnp.float32), norm_gain)
    hn_all = lax.all_gather(norm_loc.astype(jnp.bfloat16), 'tp', axis=1, tiled=True)
    label_all = lax.all_gather(labels, 'tp', axis=1, tiled=True)
    mask_all = lax.all_gather(loss_mask, 'tp', axis=1, tiled=True)
    logits = jnp.einsum('btd,dv->btv', hn_all, w_head, preferred_element_type=jnp.float32)
    row_max = lax.pmax(jnp.max(logits, axis=-1), 'tp')
    sum_exp = lax.psum(jnp.sum(jnp.exp(logits - row_max[..., None]), axis=-1), 'tp')
    col_start = lax.axis_index('tp') * v_loc
    is_label = (lax.broadcasted_iota(jnp.int32, (1, 1, v_loc), 2) + col_start) == label_all[..., None]
    label_logit = lax.psum(jnp.sum(jnp.where(is_label, logits, 0.0), axis=-1), 'tp')
    log_norm = row_max + jnp.log(sum_exp)
    tok_weight = mask_all.astype(jnp.float32)
    kept_count = jnp.sum(tok_weight)
    mean_loss = jnp.sum(tok_weight * (log_norm - label_logit)) / kept_count
    tok_scale = tok_weight / kept_count
    d_logits = ((jnp.exp(logits - log_norm[..., None]) - is_label.astype(jnp.float32)) * tok_scale[..., None]).astype(jnp.bfloat16)
    d_head = jnp.einsum('btd,btv->dv', hn_all, d_logits, preferred_element_type=jnp.float32).astype(jnp.bfloat16)
    dhn_part = jnp.einsum('btv,dv->btd', d_logits, w_head, preferred_element_type=jnp.float32).astype(jnp.bfloat16)
    received = lax.all_to_all(dhn_part.reshape(batch_size, n_shards, seq_loc, model_width), 'tp', 1, 1, tiled=True)
    d_norm = jnp.sum(received, axis=1, dtype=jnp.float32)
    d_x, d_gain = norm_vjp(d_norm)
    d_gain = lax.psum(d_gain, 'tp')
    return mean_loss, d_x.astype(jnp.bfloat16), d_head, d_gain


def solution(mesh):
    n = mesh.shape['tp']
    dims = (n // 8, 2, 2, 2)
    bits = [1 << i for i in range(n.bit_length() - 1)]

    def swap(a, flip):
        return lax.ppermute(a, 'tp', [(i, i ^ flip) for i in range(n)])

    def at(a, axis, i):
        return lax.dynamic_index_in_dim(a, i, axis, keepdims=False)

    def after(values, dep):
        return lax.optimization_barrier((values, dep))[0]

    def device_step(hidden, labels, loss_mask, norm_gain, w_head):
        f32, i32 = jnp.float32, jnp.int32
        batch_size, seq_loc, model_width = hidden.shape
        n_rows = batch_size * seq_loc
        v_loc = w_head.shape[1]
        me = lax.axis_index('tp')
        place = {'core': me & 1, 'x': (me >> 1) & 1, 'y': (me >> 2) & 1, 'z': me >> 3}
        slot = jnp.arange(n_rows, dtype=i32)

        mask = loss_mask.reshape(n_rows)
        pos = jnp.cumsum(mask) - 1
        all_slots = jnp.arange(n_rows, dtype=i32)
        chosen = (pos[None, :] == all_slots[:, None]) & (mask[None, :] == 1)
        order = jnp.sum(jnp.where(chosen, all_slots[None, :], 0), axis=1)
        packed_lab = jnp.sum(jnp.where(chosen, labels.reshape(n_rows)[None, :] + 1, 0), axis=1) - 1
        packed = jnp.take(hidden.reshape(n_rows, model_width), order, axis=0, mode='clip')
        count = jnp.maximum(jnp.sum(mask) - ROWS[0], 0)
        n_rest = n_rows - ROWS[0]
        slot = jnp.arange(n_rest, dtype=i32)

        def normed(x_rows):
            out, vjp = jax.vjp(rms_norm, x_rows.astype(f32), norm_gain)
            out = out.astype(jnp.bfloat16)
            return lax.all_gather(out, 'tp', axis=0, tiled=True), vjp, out

        hn, vjps = [None, None], [None, None]
        hn[0], vjps[0], sent = normed(packed[:ROWS[0]])
        rows, lab = after((packed[ROWS[0]:], packed_lab[ROWS[0]:]), sent)
        fits = jnp.bool_(True)
        moves = []
        for bit, cap in STAGES:
            start = jnp.maximum(count - cap, 0)
            ints = jnp.concatenate([lax.dynamic_slice_in_dim(lab, start, cap), jnp.full((128,), count, i32)])
            got_rows = swap(lax.dynamic_slice_in_dim(rows, start, cap), bit)
            got_ints = swap(ints, bit)
            other = got_ints[cap]
            upper = (me & bit) // bit
            target = (count + other + 1 - upper) >> 1
            fits = fits & (jnp.abs(target - count) <= cap)
            first = count + other - target - jnp.maximum(other - cap, 0)
            src = jnp.where(slot < count, slot, n_rest + jnp.clip(first + slot - count, 0, cap - 1))
            rows = jnp.take(jnp.concatenate([rows, got_rows]), src, axis=0, mode='clip')
            lab = jnp.take(jnp.concatenate([lab, got_ints[:cap]]), src, axis=0, mode='clip')
            moves.append((bit, cap, count, other, target))
            count = target
        fits = fits & (count <= ROWS[1])
        hn[1], vjps[1], _ = normed(rows[:ROWS[1]])
        lab = jnp.where(slot < count, lab, -1)[:ROWS[1]]
        rows_all = sum(ROWS)
        known = lax.all_gather(jnp.concatenate([packed_lab[:ROWS[0]], lab, jnp.full((128,), fits.astype(i32))]), 'tp', axis=0, tiled=False)
        all_fit = jnp.min(known[:, rows_all]) == 1
        label_all = [k.reshape(-1) for k in jnp.split(known[:, :rows_all], [ROWS[0]], axis=1)]
        weight = [(lb >= 0).astype(f32) for lb in label_all]
        kept_count = sum(jnp.sum(w) for w in weight)
        cols = lax.broadcasted_iota(i32, (1, v_loc), 1) + me * v_loc

        def forward(c):
            lg = jnp.einsum('td,dv->tv', hn[c], w_head, preferred_element_type=f32)
            lg = lax.optimization_barrier(lg)
            row_max = jnp.max(lg, axis=-1)
            row_sum = jnp.sum(jnp.exp(lg - row_max[:, None]), axis=-1)
            row_lab = jnp.sum(jnp.where(cols == label_all[c][:, None], lg, 0.0), axis=-1)
            return lg, jnp.stack([row_max, row_sum, row_lab])

        def combine_all(mine):
            for bit in bits:
                theirs = swap(mine, bit)
                upper = (me & bit) != 0
                lo, hi = jnp.where(upper, theirs, mine), jnp.where(upper, mine, theirs)
                top = jnp.maximum(lo[0], hi[0])
                mine = jnp.stack([top, lo[1] * jnp.exp(lo[0] - top) + hi[1] * jnp.exp(hi[0] - top), lo[2] + hi[2]])
            return mine[0] + jnp.log(mine[1]), mine[2]

        def softmax_grad(c, lg, log_norm):
            is_label = (cols == label_all[c][:, None]).astype(f32)
            scale = weight[c] / kept_count
            return ((jnp.exp(lg - log_norm[:, None]) - is_label) * scale[:, None]).astype(jnp.bfloat16)

        class Reduce:
            def __init__(self, part, path, per):
                part = part.reshape(*dims, per, -1)
                step = {'x': 2, 'y': 4}
                a, self.second_axis, self.third_axis = path
                a_axis = {'y': 1, 'x': 2}[a]
                self.bit = {**step, 'z': 8}

                def group(da, dc):
                    return at(at(part, 3, place['core'] ^ dc), a_axis, place[a] ^ da)

                self.sent = [group(1, 0), group(1, 1), group(0, 1)]
                self.terms = [group(0, 0)]
                self.terms += [swap(g, f) for g, f in zip(self.sent, (step[a], step[a] | 1, 1))]

            def _exchange(self, pick, name):
                size = dims[0] if name == 'z' else 2
                self.sent = [pick(place[name] ^ d) for d in range(1, size)]
                self.terms = [pick(place[name])]
                self.terms += [swap(g, self.bit[name] * d) for d, g in enumerate(self.sent, 1)]
                return self.sent

            def second(self, dep):
                terms, name = after(self.terms, dep), self.second_axis
                axis = 0 if name == 'z' else 1
                return self._exchange(lambda i: sum(at(t, axis, i).astype(f32) for t in terms), name)

            def third(self, dep):
                terms = after(self.terms, dep)
                return self._exchange(lambda i: sum(at(t, 0, i) for t in terms), self.third_axis)

            def last(self, dep):
                return sum(after(self.terms, dep))

        d_logits, log_norm, label_logit, units = {}, {}, {}, {}

        def hidden_grad(c, u, dep):
            low = sum(w for _, w in UNITS[:u]) * model_width // 32
            path, w = UNITS[u]
            dl, w_part = after(d_logits[c], dep), w_head[low:low + w * model_width // 32]
            part = jnp.einsum('tv,dv->td', dl, w_part, preferred_element_type=f32).astype(jnp.bfloat16)
            units[c, u] = Reduce(part, path, ROWS[c])
            return units[c, u].sent

        def head_grad(c, acc, dep):
            dl = after(d_logits[c], dep)
            term = jnp.einsum('td,tv->dv', hn[c], dl, preferred_element_type=f32)
            return term if acc is None else acc + term

        nu = len(UNITS)
        lg0, st0 = forward(0)
        log_norm[0], label_logit[0] = combine_all(st0)
        d_logits[0] = dep = softmax_grad(0, lg0, log_norm[0])
        for u in range(nu):
            dep = hidden_grad(0, u, dep)
        dep = units[0, 0].second(dep)
        dep = units[0, 1].second(dep)
        hn[1] = after(hn[1], dep)
        lg1, st1 = forward(1)
        log_norm[1], label_logit[1] = combine_all(st1)
        dep = units[0, 2].second(log_norm[1])
        dep = units[0, 3].second(dep)
        dep = units[0, 0].third(dep)
        dep = units[0, 1].third(dep)
        d_logits[1] = dep = softmax_grad(1, after(lg1, dep), log_norm[1])
        dep = hidden_grad(1, 0, dep)
        dep = hidden_grad(1, 1, dep)
        dep = units[0, 2].third(dep)
        dep = units[0, 3].third(dep)
        dep = hidden_grad(1, 2, dep)
        dep = hidden_grad(1, 3, dep)
        dep = units[1, 0].second(dep)
        dep = units[1, 1].second(dep)
        head = dep = head_grad(0, None, dep)
        dep = units[1, 2].second(dep)
        dep = units[1, 3].second(dep)
        early = vjps[0](jnp.concatenate([units[0, u].last(dep) for u in range(nu)], axis=-1))
        dep = early = early[0].astype(jnp.bfloat16), early[1]
        for u in range(nu):
            dep = units[1, u].third(dep)
        d_head = dep = head_grad(1, head, dep).astype(jnp.bfloat16)
        late = vjps[1](jnp.concatenate([units[1, u].last(dep) for u in range(nu)], axis=-1))
        d_x, d_gain = (early[0], late[0].astype(jnp.bfloat16)), early[1] + late[1]
        loss = sum(jnp.sum(weight[c] * (log_norm[c] - label_logit[c])) for c in range(2))
        mean_loss = loss / kept_count
        for bit in bits:
            d_gain = d_gain + swap(d_gain, bit)

        back = jnp.concatenate([d_x[1], jnp.zeros((n_rest - ROWS[1], model_width), jnp.bfloat16)])
        for bit, cap, count, other, target in reversed(moves):
            got = swap(lax.dynamic_slice_in_dim(back, jnp.minimum(count, n_rest - cap), cap), bit)
            first = jnp.maximum(other - (n_rest - cap), 0)
            src = jnp.where(slot < target, slot, n_rest + jnp.clip(first + slot - target, 0, cap - 1))
            back = jnp.take(jnp.concatenate([back, got]), src, axis=0, mode='clip')
        back = jnp.take(jnp.concatenate([d_x[0], back]), pos, axis=0, mode='clip')
        d_hidden = jnp.where(mask[:, None] == 1, back, jnp.zeros((), jnp.bfloat16)).reshape(hidden.shape)

        def every_token(_):
            return (jnp.bool_(True), *full_step(n, hidden, labels, loss_mask, norm_gain, w_head))

        return lax.while_loop(lambda c: ~c[0], every_token, (all_fit, mean_loss, d_hidden, d_head, d_gain))[1:]

    return jax.shard_map(device_step, mesh=mesh, in_specs=(P(None, 'tp', None), P(None, 'tp'), P(None, 'tp'), P(), P(None, 'tp')), out_specs=(P(), P(None, 'tp', None), P(None, 'tp'), P()), check_vma=False)
```

```python
import jax
import jax.numpy as jnp
from jax import lax
from jax.sharding import PartitionSpec as P

NORM_EPS = 1e-6
STAGES = ((1, 72), (2, 56), (4, 40), (8, 32), (16, 24))
ROWS = (56, 64)
UNITS = ((('y', 'z', 'x'), 6), (('x', 'z', 'y'), 6), (('x', 'y', 'z'), 10), (('y', 'x', 'z'), 10))


def rms_norm(x_rows, norm_gain):
    inv_rms = lax.rsqrt(jnp.mean(x_rows * x_rows, axis=-1, keepdims=True) + NORM_EPS)
    return x_rows * inv_rms * norm_gain


def full_step(n_shards, hidden, labels, loss_mask, norm_gain, w_head):
    batch_size, seq_loc, model_width = hidden.shape
    v_loc = w_head.shape[1]
    norm_loc, norm_vjp = jax.vjp(rms_norm, hidden.astype(jnp.float32), norm_gain)
    hn_all = lax.all_gather(norm_loc.astype(jnp.bfloat16), 'tp', axis=1, tiled=True)
    label_all = lax.all_gather(labels, 'tp', axis=1, tiled=True)
    mask_all = lax.all_gather(loss_mask, 'tp', axis=1, tiled=True)
    logits = jnp.einsum('btd,dv->btv', hn_all, w_head, preferred_element_type=jnp.float32)
    row_max = lax.pmax(jnp.max(logits, axis=-1), 'tp')
    sum_exp = lax.psum(jnp.sum(jnp.exp(logits - row_max[..., None]), axis=-1), 'tp')
    col_start = lax.axis_index('tp') * v_loc
    is_label = (lax.broadcasted_iota(jnp.int32, (1, 1, v_loc), 2) + col_start) == label_all[..., None]
    label_logit = lax.psum(jnp.sum(jnp.where(is_label, logits, 0.0), axis=-1), 'tp')
    log_norm = row_max + jnp.log(sum_exp)
    tok_weight = mask_all.astype(jnp.float32)
    kept_count = jnp.sum(tok_weight)
    mean_loss = jnp.sum(tok_weight * (log_norm - label_logit)) / kept_count
    tok_scale = tok_weight / kept_count
    d_logits = ((jnp.exp(logits - log_norm[..., None]) - is_label.astype(jnp.float32)) * tok_scale[..., None]).astype(jnp.bfloat16)
    d_head = jnp.einsum('btd,btv->dv', hn_all, d_logits, preferred_element_type=jnp.float32).astype(jnp.bfloat16)
    dhn_part = jnp.einsum('btv,dv->btd', d_logits, w_head, preferred_element_type=jnp.float32).astype(jnp.bfloat16)
    received = lax.all_to_all(dhn_part.reshape(batch_size, n_shards, seq_loc, model_width), 'tp', 1, 1, tiled=True)
    d_norm = jnp.sum(received, axis=1, dtype=jnp.float32)
    d_x, d_gain = norm_vjp(d_norm)
    d_gain = lax.psum(d_gain, 'tp')
    return mean_loss, d_x.astype(jnp.bfloat16), d_head, d_gain


def solution(mesh):
    n = mesh.shape['tp']
    dims = (n // 8, 2, 2, 2)
    bits = [1 << i for i in range(n.bit_length() - 1)]

    def swap(a, flip):
        return lax.ppermute(a, 'tp', [(i, i ^ flip) for i in range(n)])

    def at(a, axis, i):
        return lax.dynamic_index_in_dim(a, i, axis, keepdims=False)

    def in_order(rows):
        return jnp.take(rows, jnp.arange(n, dtype=jnp.int32) ^ lax.axis_index('tp'), axis=0, mode='clip')

    def gather_small(a):
        rows = a[None]
        for bit in bits:
            rows = jnp.concatenate([rows, swap(rows, bit)])
        return in_order(rows)

    def after(values, dep):
        return lax.optimization_barrier((values, dep))[0]

    def device_step(hidden, labels, loss_mask, norm_gain, w_head):
        f32, i32 = jnp.float32, jnp.int32
        batch_size, seq_loc, model_width = hidden.shape
        n_rows = batch_size * seq_loc
        v_loc = w_head.shape[1]
        me = lax.axis_index('tp')
        place = {'core': me & 1, 'x': (me >> 1) & 1, 'y': (me >> 2) & 1, 'z': me >> 3}
        slot = jnp.arange(n_rows, dtype=i32)

        mask = loss_mask.reshape(n_rows)
        pos = jnp.cumsum(mask) - 1
        all_slots = jnp.arange(n_rows, dtype=i32)
        chosen = (pos[None, :] == all_slots[:, None]) & (mask[None, :] == 1)
        order = jnp.sum(jnp.where(chosen, all_slots[None, :], 0), axis=1)
        packed_lab = jnp.sum(jnp.where(chosen, labels.reshape(n_rows)[None, :] + 1, 0), axis=1) - 1
        packed = jnp.take(hidden.reshape(n_rows, model_width), order, axis=0, mode='clip')
        kept = jnp.sum(mask)
        count = jnp.maximum(kept - ROWS[0], 0)
        n_rest = n_rows - ROWS[0]
        slot = jnp.arange(n_rest, dtype=i32)

        def normed(x_rows):
            out, vjp = jax.vjp(rms_norm, x_rows.astype(f32), norm_gain)
            out = out.astype(jnp.bfloat16)
            return lax.all_gather(out, 'tp', axis=0, tiled=True), vjp, out

        hn, vjps = [None, None], [None, None]
        hn[0], vjps[0], sent = normed(packed[:ROWS[0]])
        rows, lab = after((packed[ROWS[0]:], packed_lab[ROWS[0]:]), sent)
        known = jnp.concatenate([packed_lab[:ROWS[0]], jnp.full((128 - ROWS[0],), kept, i32)])
        fits = jnp.bool_(True)
        moves = []
        for bit, cap in STAGES:
            start = jnp.maximum(count - cap, 0)
            ints = jnp.concatenate([known, jnp.full((128,), count, i32), lax.dynamic_slice_in_dim(lab, start, cap)])
            got_rows = swap(lax.dynamic_slice_in_dim(rows, start, cap), bit)
            got_ints = swap(ints, bit)
            size = known.shape[0]
            known = jnp.concatenate([known, got_ints[:size]])
            other, got_lab = got_ints[size], got_ints[size + 128:]
            upper = (me & bit) // bit
            target = (count + other + 1 - upper) >> 1
            fits = fits & (jnp.abs(target - count) <= cap)
            first = count + other - target - jnp.maximum(other - cap, 0)
            src = jnp.where(slot < count, slot, n_rest + jnp.clip(first + slot - count, 0, cap - 1))
            rows = jnp.take(jnp.concatenate([rows, got_rows]), src, axis=0, mode='clip')
            lab = jnp.take(jnp.concatenate([lab, got_lab]), src, axis=0, mode='clip')
            moves.append((bit, cap, count, other, target))
            count = target
        known = in_order(known.reshape(n, 128))
        label_all = [known[:, :ROWS[0]].reshape(-1)]
        kept_count = jnp.sum(known[:, ROWS[0]]).astype(f32)
        fits = fits & (count <= ROWS[1])
        hn[1], vjps[1], _ = normed(rows[:ROWS[1]])
        lab = jnp.where(slot < count, lab, -1)[:ROWS[1]]
        known = gather_small(jnp.concatenate([lab, jnp.full((128 - ROWS[1],), fits.astype(i32))]))
        label_all.append(known[:, :ROWS[1]].reshape(-1))
        all_fit = jnp.min(known[:, ROWS[1]]) == 1
        weight = [(lb >= 0).astype(f32) for lb in label_all]
        cols = lax.broadcasted_iota(i32, (1, v_loc), 1) + me * v_loc

        def forward(c):
            lg = jnp.einsum('td,dv->tv', hn[c], w_head, preferred_element_type=f32)
            lg = lax.optimization_barrier(lg)
            row_max = jnp.max(lg, axis=-1)
            row_sum = jnp.sum(jnp.exp(lg - row_max[:, None]), axis=-1)
            row_lab = jnp.sum(jnp.where(cols == label_all[c][:, None], lg, 0.0), axis=-1)
            return lg, jnp.stack([row_max, row_sum, row_lab])

        def combine_all(mine):
            for bit in bits:
                theirs = swap(mine, bit)
                upper = (me & bit) != 0
                lo, hi = jnp.where(upper, theirs, mine), jnp.where(upper, mine, theirs)
                top = jnp.maximum(lo[0], hi[0])
                mine = jnp.stack([top, lo[1] * jnp.exp(lo[0] - top) + hi[1] * jnp.exp(hi[0] - top), lo[2] + hi[2]])
            return mine[0] + jnp.log(mine[1]), mine[2]

        def softmax_grad(c, lg, log_norm):
            is_label = (cols == label_all[c][:, None]).astype(f32)
            scale = weight[c] / kept_count
            return ((jnp.exp(lg - log_norm[:, None]) - is_label) * scale[:, None]).astype(jnp.bfloat16)

        class Reduce:
            def __init__(self, part, path, per):
                part = part.reshape(*dims, per, -1)
                step = {'x': 2, 'y': 4}
                a, self.second_axis, self.third_axis = path
                a_axis = {'y': 1, 'x': 2}[a]
                self.bit = {**step, 'z': 8}

                def group(da, dc):
                    return at(at(part, 3, place['core'] ^ dc), a_axis, place[a] ^ da)

                self.sent = [group(1, 0), group(1, 1), group(0, 1)]
                self.terms = [group(0, 0)]
                self.terms += [swap(g, f) for g, f in zip(self.sent, (step[a], step[a] | 1, 1))]

            def _exchange(self, pick, name):
                size = dims[0] if name == 'z' else 2
                self.sent = [pick(place[name] ^ d) for d in range(1, size)]
                self.terms = [pick(place[name])]
                self.terms += [swap(g, self.bit[name] * d) for d, g in enumerate(self.sent, 1)]
                return self.sent

            def second(self, dep):
                terms, name = after(self.terms, dep), self.second_axis
                axis = 0 if name == 'z' else 1
                return self._exchange(lambda i: sum(at(t, axis, i).astype(f32) for t in terms), name)

            def third(self, dep):
                terms = after(self.terms, dep)
                return self._exchange(lambda i: sum(at(t, 0, i) for t in terms), self.third_axis)

            def last(self, dep):
                return sum(after(self.terms, dep))

        d_logits, log_norm, label_logit, units = {}, {}, {}, {}

        def hidden_grad(c, u, dep):
            low = sum(w for _, w in UNITS[:u]) * model_width // 32
            path, w = UNITS[u]
            dl, w_part = after(d_logits[c], dep), w_head[low:low + w * model_width // 32]
            part = jnp.einsum('tv,dv->td', dl, w_part, preferred_element_type=f32).astype(jnp.bfloat16)
            units[c, u] = Reduce(part, path, ROWS[c])
            return units[c, u].sent

        def head_grad(c, acc, dep):
            dl = after(d_logits[c], dep)
            term = jnp.einsum('td,tv->dv', hn[c], dl, preferred_element_type=f32)
            return term if acc is None else acc + term

        nu = len(UNITS)
        lg0, st0 = forward(0)
        log_norm[0], label_logit[0] = combine_all(st0)
        d_logits[0] = dep = softmax_grad(0, lg0, log_norm[0])
        for u in range(nu):
            dep = hidden_grad(0, u, dep)
        dep = units[0, 0].second(dep)
        dep = units[0, 1].second(dep)
        hn[1] = after(hn[1], dep)
        lg1, st1 = forward(1)
        log_norm[1], label_logit[1] = combine_all(st1)
        dep = units[0, 2].second(log_norm[1])
        dep = units[0, 3].second(dep)
        dep = units[0, 0].third(dep)
        dep = units[0, 1].third(dep)
        d_logits[1] = dep = softmax_grad(1, after(lg1, dep), log_norm[1])
        dep = hidden_grad(1, 0, dep)
        dep = hidden_grad(1, 1, dep)
        dep = units[0, 2].third(dep)
        dep = units[0, 3].third(dep)
        dep = hidden_grad(1, 2, dep)
        dep = hidden_grad(1, 3, dep)
        dep = units[1, 0].second(dep)
        dep = units[1, 1].second(dep)
        head = dep = head_grad(0, None, dep)
        dep = units[1, 2].second(dep)
        dep = units[1, 3].second(dep)
        early = vjps[0](jnp.concatenate([units[0, u].last(dep) for u in range(nu)], axis=-1))
        dep = early = early[0].astype(jnp.bfloat16), early[1]
        for u in range(nu):
            dep = units[1, u].third(dep)
        d_head = dep = head_grad(1, head, dep).astype(jnp.bfloat16)
        late = vjps[1](jnp.concatenate([units[1, u].last(dep) for u in range(nu)], axis=-1))
        d_x, d_gain = (early[0], late[0].astype(jnp.bfloat16)), early[1] + late[1]
        loss = sum(jnp.sum(weight[c] * (log_norm[c] - label_logit[c])) for c in range(2))
        mean_loss = loss / kept_count

        room = n_rest - ROWS[1] + max(cap for _, cap in STAGES)
        back = jnp.concatenate([*d_x, jnp.zeros((room, model_width), jnp.bfloat16)])
        for bit, cap, count, other, target in reversed(moves):
            got = swap(lax.dynamic_slice_in_dim(back, ROWS[0] + count, cap), bit)
            d_gain = d_gain + swap(d_gain, bit)
            back = lax.dynamic_update_slice_in_dim(back, got, ROWS[0] + target, 0)
            back, d_gain = lax.optimization_barrier((back, d_gain))
        back = jnp.take(back, pos, axis=0, mode='clip')
        d_hidden = jnp.where(mask[:, None] == 1, back, jnp.zeros((), jnp.bfloat16)).reshape(hidden.shape)

        def every_token(_):
            return (jnp.bool_(True), *full_step(n, hidden, labels, loss_mask, norm_gain, w_head))

        return lax.while_loop(lambda c: ~c[0], every_token, (all_fit, mean_loss, d_hidden, d_head, d_gain))[1:]

    return jax.shard_map(device_step, mesh=mesh, in_specs=(P(None, 'tp', None), P(None, 'tp'), P(None, 'tp'), P(), P(None, 'tp')), out_specs=(P(), P(None, 'tp', None), P(None, 'tp'), P()), check_vma=False)
```
